256 devices in a mesh: island: 8 (over y, core), section: 4 (over z_hi), tensor: 8 (over z_lo, x).
Axes of the slice: x: 4, y: 4, z: 8 (z_hi: 4, z_lo: 2; z = z_hi * 2 + z_lo), core: 2. Of those that a mesh axis runs over, the one named last changes fastest.
Arguments:
- hidden: bfloat16 [8, 4, 256, 8192], P('island', 'section', 'tensor'), may hold values from -6 to 6
- norm_gain: bfloat16 [4, 8192], P('section'), may hold values from 0.099609375 to 1.8984375
- grad_above: bfloat16 [8, 256, 8192], P('island', 'tensor'), may hold values from -6 to 6
- key_cot: bfloat16 [8, 4, 256, 1024], P('island', 'section', None, 'tensor'), may hold values from -6 to 6
- value_cot: bfloat16 [8, 4, 256, 1024], P('island', 'section', None, 'tensor'), may hold values from -6 to 6
- local_key: bfloat16 [8, 4, 8192, 1024], P('island', 'section', None, 'tensor'), may hold values from -6 to 6
- local_value: bfloat16 [8, 4, 8192, 1024], P('island', 'section', None, 'tensor'), may hold values from -6 to 6
- anchor_key: float32 [4, 8192, 1024], P('section', 'island', 'tensor'), may hold values from -6 to 6
- anchor_value: float32 [4, 8192, 1024], P('section', 'island', 'tensor'), may hold values from -6 to 6
- momentum_key: float32 [4, 8192, 1024], P('section', 'island', 'tensor'), may hold values from -4 to 4
- momentum_value: float32 [4, 8192, 1024], P('section', 'island', 'tensor'), may hold values from -4 to 4
Outputs:
- anchor_key_new: float32 [4, 8192, 1024], P('section', 'island', 'tensor')
- anchor_value_new: float32 [4, 8192, 1024], P('section', 'island', 'tensor')
- momentum_key_new: float32 [4, 8192, 1024], P('section', 'island', 'tensor')
- momentum_value_new: float32 [4, 8192, 1024], P('section', 'island', 'tensor')
- input_grad: bfloat16 [8, 4, 256, 8192], P('island', 'section', 'tensor')
The draws below stay inside these ranges and needn't reach their ends.
All inputs are finite; a program needn't handle non-finite values.
Results may differ from the reference program's by a relative error of at most 0.024.
Values may be sent and summed in bfloat16 or wider, within the bound.
A program may use at most 64 MiB of HBM per device.

```python
import jax
import jax.numpy as jnp
from jax import lax

D = 8192
TOK = 256
KV = 1024
ISLANDS = 8
SECTIONS = 4
N_ISLAND = 8
N_SECTION = 4
N_TENSOR = 8


def raised(entries, stream_key, source, target, shards_of, factor):
    owner, partner = [(jnp.arange(entries.shape[dim]) // (entries.shape[dim] // shards_of)).reshape([-1 if axis == dim else 1 for axis in range(entries.ndim)]) for dim in (source, target)]
    chosen = jax.random.permutation(stream_key, shards_of)[partner]
    strong = (owner == chosen) | (owner == (partner + shards_of // 2) % shards_of)
    return jnp.where(strong, factor * entries, entries)


def steps_of(rng, dims, cuts, smallest, top_value):
    factor_of, own = 1.0, jax.random.fold_in(rng, 6)
    for axis_at, shards_of in cuts:
        heights = jnp.exp(jax.random.uniform(jax.random.fold_in(own, axis_at), (shards_of,), jnp.float32, smallest / len(cuts), top_value / len(cuts)))
        factor_of = factor_of * jnp.repeat(heights, dims[axis_at] // shards_of).reshape([-1 if axis == axis_at else 1 for axis in range(len(dims))])
    return factor_of


def centred(key, dims, spread, reach, shards=(), kind=jnp.bfloat16):
    values = jax.random.normal(key, dims, jnp.float32) * spread
    if len(shards) > 0:
        values = steps_of(key, dims, shards, -0.22, 0.18) * values
    return jnp.clip(values, min=-reach, max=reach).astype(kind)


def gaussian_with(stream_key, dims, scale, most, pieces, heavy, kind=jnp.bfloat16):
    result = scale * jax.random.normal(stream_key, dims, jnp.float32)
    if pieces:
        result = result * steps_of(stream_key, dims, pieces, -0.22, 0.18)
    return jnp.clip(raised(result, jax.random.fold_in(stream_key, 3), *heavy), -most, most).astype(kind)


def setup_inputs(seed: int = 0) -> dict:
    splits = jax.random.split(jax.random.key(seed), 12)
    hidden = centred(splits[0], (ISLANDS, SECTIONS, TOK, D), 1.0, 6.0, ((0, 8), (1, 4), (2, 8)))
    norm_gain = jnp.clip(1.0 + 0.18 * jax.random.normal(splits[1], (SECTIONS, D), jnp.float32), 0.099609375, 1.8984375).astype(jnp.bfloat16)
    grad_above = centred(splits[2], (ISLANDS, TOK, D), 1.0, 6.0, ((0, 8), (1, 8)))
    key_cot = centred(splits[3], (ISLANDS, SECTIONS, TOK, KV), 1.0, 6.0, ((0, 8), (1, 4), (3, 8)))
    value_cot = centred(splits[4], (ISLANDS, SECTIONS, TOK, KV), 1.0, 6.0, ((0, 8), (1, 4), (3, 8)))
    local_key = gaussian_with(splits[5], (ISLANDS, SECTIONS, D, KV), 1.0, 6.0, ((0, 8), (1, 4), (3, 8)), (0, 2, 8, 2.0))
    local_value = gaussian_with(splits[6], (ISLANDS, SECTIONS, D, KV), 1.0, 6.0, ((0, 8), (1, 4), (3, 8)), (0, 2, 8, 2.0))
    anchor_key = centred(splits[7], (SECTIONS, D, KV), 1.0, 6.0, ((0, 4), (1, 8), (2, 8)), jnp.float32)
    anchor_value = centred(splits[8], (SECTIONS, D, KV), 1.0, 6.0, ((0, 4), (1, 8), (2, 8)), jnp.float32)
    momentum_key = centred(splits[9], (SECTIONS, D, KV), 0.5, 4.0, ((0, 4), (1, 8), (2, 8)), jnp.float32)
    momentum_value = centred(splits[10], (SECTIONS, D, KV), 0.5, 4.0, ((0, 4), (1, 8), (2, 8)), jnp.float32)
    return dict(hidden=hidden, norm_gain=norm_gain, grad_above=grad_above, key_cot=key_cot, value_cot=value_cot, local_key=local_key, local_value=local_value, anchor_key=anchor_key, anchor_value=anchor_value, momentum_key=momentum_key, momentum_value=momentum_value)


epsilon = 1e-05
inner_rate = 0.5
outer_rate = 0.7
outer_beta = 0.9

def norm_parts(resid, gains):
    inverse_rms = lax.rsqrt(lax.optimization_barrier(jnp.mean(resid * resid, axis=-1, keepdims=True)) + epsilon)
    normed = (resid * inverse_rms * gains).astype(jnp.bfloat16)
    return (inverse_rms, normed)

def norm_backward(resid, inverse_rms, gains, upstream):
    scaled = gains * upstream
    return inverse_rms * scaled - resid * inverse_rms ** 3 * lax.optimization_barrier(jnp.mean(resid * scaled, axis=-1, keepdims=True))

def contract_rows(left, right):
    return lax.dot_general(left, right, (((0,), (0,)), ((), ())), preferred_element_type=jnp.float32)

def contract_cols(left, right):
    return lax.dot_general(left, right, (((1,), (1,)), ((), ())), preferred_element_type=jnp.float32)

def outer_update(anchor, momentum, mean_delta):
    momentum_new = outer_beta * momentum + mean_delta
    return (anchor - outer_rate * (mean_delta + outer_beta * momentum_new), momentum_new)

def reference(hidden, norm_gain, grad_above, key_cot, value_cot, local_key, local_value, anchor_key, anchor_value, momentum_key, momentum_value):
    factor = float(D) ** (-0.5)
    width = KV // N_TENSOR
    key_sums = [jnp.zeros((D, KV), jnp.float32) for section_index in range(N_SECTION)]
    value_sums = [jnp.zeros((D, KV), jnp.float32) for section_index in range(N_SECTION)]
    grads_out = []
    for island in range(N_ISLAND):
        branches = []
        for section_index in range(N_SECTION):
            resid = hidden[island, section_index].astype(jnp.float32)
            gains = norm_gain[section_index].astype(jnp.float32)
            inverse_rms, normed = norm_parts(resid, gains)
            key_rows = key_cot[island, section_index]
            value_rows = value_cot[island, section_index]
            weight_key = local_key[island, section_index]
            weight_value = local_value[island, section_index]
            grad_key = contract_rows(normed, key_rows) * factor
            grad_value = contract_rows(normed, value_rows) * factor
            new_key = weight_key.astype(jnp.float32) - inner_rate * grad_key
            new_value = weight_value.astype(jnp.float32) - inner_rate * grad_value
            key_sums[section_index] = key_sums[section_index] + (anchor_key[section_index] - new_key)
            value_sums[section_index] = value_sums[section_index] + (anchor_value[section_index] - new_value)
            upstream = jnp.zeros((TOK, D), jnp.float32)
            for member in range(N_TENSOR):
                low = member * width
                high = low + width
                partial_value = (contract_cols(key_rows[:, low:high], weight_key[:, low:high]) + contract_cols(value_rows[:, low:high], weight_value[:, low:high])) * factor
                rounded = lax.optimization_barrier(partial_value.astype(jnp.bfloat16))
                upstream = upstream + rounded.astype(jnp.float32)
            branches.append(norm_backward(resid, inverse_rms, gains, upstream))
        running = grad_above[island].astype(jnp.float32)
        section_grads = [None] * N_SECTION
        for section_index in range(N_SECTION - 1, -1, -1):
            running = running + branches[section_index]
            section_grads[section_index] = running.astype(jnp.bfloat16)
        grads_out.append(jnp.stack(section_grads))
    input_grad = jnp.stack(grads_out)
    anchors_key, moments_key, anchors_value, moments_value = ([], [], [], [])
    for section_index in range(N_SECTION):
        new_anchor, new_moment = outer_update(anchor_key[section_index], momentum_key[section_index], key_sums[section_index] / N_ISLAND)
        anchors_key.append(new_anchor)
        moments_key.append(new_moment)
        new_anchor, new_moment = outer_update(anchor_value[section_index], momentum_value[section_index], value_sums[section_index] / N_ISLAND)
        anchors_value.append(new_anchor)
        moments_value.append(new_moment)
    return (jnp.stack(anchors_key), jnp.stack(anchors_value), jnp.stack(moments_key), jnp.stack(moments_value), input_grad)
```

```python
import types

import jax
import jax.numpy as jnp
from jax import lax
from jax.experimental import pallas as pl
from jax.experimental.pallas import tpu as pltpu
from jax.sharding import PartitionSpec as P

MESH = pl.DeviceIdType.MESH
BF = jnp.bfloat16
F32 = jnp.float32

epsilon = 1e-05
inner_rate = 0.5
outer_rate = 0.7
outer_beta = 0.9

D = 8192
TOK = 256
NX, NY, NZ, NS = 4, 4, 2, 4
HALF = D // 2
STEP = 512
NSTEP = D // STEP
PIECES = 4
PIECE = D // PIECES
FACTOR = float(D) ** (-0.5)

SCRATCH = dict(
    hid=((32, D), BF),
    gain=((1, D), BF),
    above=((32, D), BF),
    cot=((TOK, 256), BF),
    w=((4, 4, 512, 256), BF),
    anc=((2, 1024, 128), F32),
    mom=((2, 1024, 128), F32),
    inv=((32, 128), F32),
    p=((8, 2, 16, D), BF),
    xo=((2, 2, 16, D), BF),
    r1=((2, 2, 16, HALF), BF),
    xw=((2, 2, 16, D), BF),
    z1=((2, 16, D), BF),
    z2=((2, 16, D), BF),
    z2s=((2, 16, D), BF),
    scaled=((2, 16, D), F32),
    coef=((2, 16, 128), F32),
    ch=((2, 16, D), BF),
    chs=((2, 16, D), BF),
    wc=((4, 2, 512, 256), BF),
    w1=((2, 512, 256), BF),
    wy=((2, 2, 512, 256), BF),
    na=((8, 32, 1024), BF),
    ar=((8, 32, 1024), BF),
    at=((4, 2, 512, 256), BF),
    cb=((4, 2, 32, 256), BF),
    bz=((4, 2, 32, 256), BF),
    b=((4, 2, 4, 2, 32, 256), BF),
    gcs=((2, 512, 256), BF),
    gc=((2, 512, 256), BF),
    gzs=((2, 256, 256), BF),
    gz=((2, 256, 256), BF),
    own=((512, 256), F32),
)
NREMOTE = 80
NLOCAL = 16


def contract_cols(left, right):
    return lax.dot_general(left, right, (((1,), (1,)), ((), ())), preferred_element_type=F32)


def contract(left, right):
    return lax.dot_general(left, right, (((1,), (0,)), ((), ())), preferred_element_type=F32)


def lanes(v):
    total = v[:, 0:128]
    for k in range(1, v.shape[1] // 128):
        total = total + v[:, 128 * k : 128 * (k + 1)]
    return total


def at_step(q, width=STEP):
    return pl.ds(pl.multiple_of(q * width, width), width)


def loop(n, body):
    def step(q, carry):
        body(q)
        return carry

    lax.fori_loop(0, n, step, 0)


def kernel(*refs):
    (hid_h, gain_h, above_h, kc_h, vc_h, wk_h, wv_h, ak_h, av_h, mk_h, mv_h) = refs[:11]
    o_ak, o_av, o_mk, o_mv, o_ig = refs[11:16]
    s = types.SimpleNamespace(**dict(zip(SCRATCH, refs[16 : 16 + len(SCRATCH)])))
    ssem, rsem, lsem = refs[16 + len(SCRATCH) :]

    island = lax.axis_index("island")
    sec = lax.axis_index("section")
    tensor = lax.axis_index("tensor")
    y, c = island // 2, lax.rem(island, 2)
    zl, x = tensor // 4, lax.rem(tensor, 4)
    oz, oc = 1 - zl, 1 - c
    slot = y * 2 + zl

    def xdev(d):
        return {"tensor": zl * 4 + lax.rem(x + d + 4, 4)}

    def ydev(d):
        return {"island": lax.rem(y + d + 4, 4) * 2 + c}

    zdev = {"tensor": oz * 4 + x}
    cdev = {"island": y * 2 + oc}

    def slotdev(k):
        return {"island": (k // 2) * 2 + c, "tensor": lax.rem(k, 2) * 4 + x}

    count = [0]
    sent = []

    def remote(src, dst, dev, keep=True):
        k = count[0]
        count[0] += 1
        copy = pltpu.make_async_remote_copy(
            src_ref=src,
            dst_ref=dst,
            send_sem=ssem.at[k],
            recv_sem=rsem.at[k],
            device_id=dev,
            device_id_type=MESH,
        )
        if keep:
            sent.append(copy)
        return copy

    nload = [0]

    def load(src, dst):
        copy = pltpu.make_async_copy(src, dst, lsem.at[nload[0]])
        nload[0] += 1
        copy.start()
        return copy

    lw = [
        load(wk_h, s.w.at[:, :, :, pl.ds(0, 128)]),
        load(wv_h, s.w.at[:, :, :, pl.ds(128, 128)]),
    ]
    lc = [load(kc_h, s.cot.at[:, pl.ds(0, 128)]), load(vc_h, s.cot.at[:, pl.ds(128, 128)])]
    lh = [load(hid_h, s.hid), load(gain_h, s.gain)]
    late = [
        load(above_h, s.above),
        load(ak_h, s.anc.at[0]),
        load(av_h, s.anc.at[1]),
        load(mk_h, s.mom.at[0]),
        load(mv_h, s.mom.at[1]),
    ]

    barrier = pltpu.get_barrier_semaphore()
    partners = [cdev, xdev(1), xdev(-1)]
    partners += [slotdev(lax.rem(slot + d, 8)) for d in range(1, 8)]
    partners += [{"section": lax.rem(sec + 1, NS)}, {"section": lax.rem(sec + 3, NS)}]
    for dev in partners:
        pl.semaphore_signal(barrier, inc=1, device_id=dev, device_id_type=MESH)

    @pl.when(sec == NS - 1)
    def _():
        def zero(q):
            s.ch[:, :, at_step(q)] = jnp.zeros((2, 16, STEP), BF)

        loop(NSTEP, zero)

    for copy in lc:
        copy.wait()
    for xx in range(4):
        for zz in range(2):
            t = (zz * 4 + xx) * 32
            s.cb[xx, zz] = s.cot[t : t + 32, :]
    pl.semaphore_wait(barrier, len(partners))

    bzc = remote(s.cb, s.bz, zdev)
    bzc.start()

    for copy in lw:
        copy.wait()
    wcc = remote(s.w.at[:, pl.ds(oc * 2, 2)], s.wc, cdev)
    wcc.start()

    def partial(q):
        val = contract_cols(s.cot[...], s.w[q // 4, lax.rem(q, 4)]) * FACTOR
        fs = at_step(q)
        for r in range(16):
            s.p[r // 2, r % 2, :, fs] = val[16 * r : 16 * r + 16].astype(BF)

    loop(NSTEP, partial)

    fa, fb = pl.ds(0, HALF), pl.ds(HALF, HALF)
    x_r, x_l, x_2 = lax.rem(x + 1, 4), lax.rem(x + 3, 4), lax.rem(x + 2, 4)

    z1c = [remote(s.p.at[oz * 4 + x_2, h], s.z1.at[h], zdev) for h in range(2)]
    xoc = [
        [
            remote(s.p.at[oz * 4 + x_r, h], s.xo.at[0, h], xdev(1)),
            remote(s.p.at[oz * 4 + x_l, h], s.xo.at[1, h], xdev(-1)),
        ]
        for h in range(2)
    ]
    nac = [
        [
            remote(s.p.at[zl * 4 + x_r, h, :, fb], s.xw.at[0, h, :, fb], xdev(1)),
            remote(s.p.at[zl * 4 + x_l, h, :, fa], s.xw.at[1, h, :, fa], xdev(-1)),
        ]
        for h in range(2)
    ]
    r1c = [
        [
            remote(s.p.at[zl * 4 + x_2, h, :, fa], s.r1.at[0, h], xdev(1)),
            remote(s.p.at[zl * 4 + x_2, h, :, fb], s.r1.at[1, h], xdev(-1)),
        ]
        for h in range(2)
    ]
    agc = [
        [
            remote(s.p.at[zl * 4 + x_r, h, :, fa], s.xw.at[0, h, :, fa], xdev(1)),
            remote(s.p.at[zl * 4 + x_l, h, :, fb], s.xw.at[1, h, :, fb], xdev(-1)),
        ]
        for h in range(2)
    ]
    z2c = [remote(s.z2s.at[h], s.z2.at[h], zdev) for h in range(2)]

    def start_direct(h):
        for copy in xoc[h] + nac[h]:
            copy.start()

    def far_block(h):
        z1c[h].wait_recv()

        def add(q):
            fs = at_step(q)
            s.p[zl * 4 + x_2, h, :, fs] = (
                s.p[zl * 4 + x_2, h, :, fs].astype(F32) + s.z1[h, :, fs].astype(F32)
            ).astype(BF)

        loop(NSTEP, add)
        for copy in r1c[h]:
            copy.start()

    def aggregate(h):
        for d, (xi, off) in enumerate(((x_r, 0), (x_l, HALF))):
            r1c[h][d].wait_recv()

            def add(q):
                src = pl.ds(pl.multiple_of(q * STEP, STEP), STEP)
                fs = pl.ds(pl.multiple_of(off + q * STEP, STEP), STEP)
                s.p[zl * 4 + xi, h, :, fs] = (
                    s.p[zl * 4 + xi, h, :, fs].astype(F32) + s.r1[d, h, :, src].astype(F32)
                ).astype(BF)

            loop(NSTEP // 2, add)
            agc[h][d].start()

    def send_across(h):
        for copy in xoc[h]:
            copy.wait_recv()

        def add(q):
            fs = at_step(q)
            s.z2s[h, :, fs] = (
                s.p[oz * 4 + x, h, :, fs].astype(F32)
                + s.xo[0, h, :, fs].astype(F32)
                + s.xo[1, h, :, fs].astype(F32)
            ).astype(BF)

        loop(NSTEP, add)
        z2c[h].start()

    z1c[0].start()
    start_direct(0)
    z1c[1].start()

    for copy in lh:
        copy.wait()

    def square(q, acc):
        seg = s.hid[:, at_step(q)].astype(F32)
        return acc + lanes(seg * seg)

    squares = lax.fori_loop(0, NSTEP, square, jnp.zeros((32, 128), F32))
    inverse = lax.rsqrt(jnp.sum(squares, axis=1, keepdims=True) / D + epsilon)
    s.inv[...] = jnp.broadcast_to(inverse, (32, 128))

    def norm(q):
        fs = at_step(q)
        inv = s.inv[:, 0:1]
        val = s.hid[:, fs].astype(F32) * inv * s.gain[:, fs].astype(F32)
        lane = pl.ds(pl.multiple_of(lax.rem(q // 2, 2) * STEP, STEP), STEP)
        s.na[(q // 4) * 2 + lax.rem(q, 2), :, lane] = val.astype(BF)

    loop(NSTEP, norm)
    ac = []
    for d in range(1, 8):
        k = lax.rem(slot + d, 8)
        copy = remote(s.na.at[k], s.ar.at[slot], slotdev(k))
        copy.start()
        ac.append(copy)
    s.ar[slot] = s.na[slot]

    bc = []
    for d in range(1, 4):
        copy = remote(s.cb, s.b.at[y, zl], ydev(d))
        copy.start()
        bc.append(copy)
    s.b[y, zl] = s.cb[...]
    bzc.wait_recv()
    for d in range(1, 4):
        copy = remote(s.bz, s.b.at[y, oz], ydev(d))
        copy.start()
        bc.append(copy)
    s.b[y, oz] = s.bz[...]

    far_block(0)

    wcc.wait_recv()

    def pair(q):
        yy, hh = q // 4, lax.rem(q // 2, 2)
        rows = pl.ds(pl.multiple_of(lax.rem(q, 2) * 256, 256), 256)
        s.w[yy, c * 2 + hh, rows, :] = (
            s.w[yy, c * 2 + hh, rows, :].astype(F32) + s.wc[yy, hh, rows, :].astype(F32)
        ).astype(BF)

    loop(16, pair)
    y_r, y_l, y_2 = lax.rem(y + 1, 4), lax.rem(y + 3, 4), lax.rem(y + 2, 4)
    w1c = [
        remote(s.w.at[y_2, c * 2], s.w1.at[0], ydev(1)),
        remote(s.w.at[y_2, c * 2 + 1], s.w1.at[1], ydev(-1)),
    ]
    wnc = [
        remote(s.w.at[y_r, c * 2 + 1], s.wy.at[0, 1], ydev(1)),
        remote(s.w.at[y_l, c * 2], s.wy.at[1, 0], ydev(-1)),
    ]
    wac = [
        remote(s.w.at[y_r, c * 2], s.wy.at[0, 0], ydev(1)),
        remote(s.w.at[y_l, c * 2 + 1], s.wy.at[1, 1], ydev(-1)),
    ]
    for copy in w1c + wnc:
        copy.start()

    aggregate(0)
    start_direct(1)
    far_block(1)

    for copy in ac:
        copy.wait_recv()

    def turn(q):
        fs = pl.ds(pl.multiple_of(q * 128, 128), 128)
        block = s.ar[:, :, fs].reshape(TOK, 128)
        rows = pl.ds(pl.multiple_of(lax.rem(q, 4) * 128, 128), 128)
        s.at[x, q // 4, rows, :] = block.T

    loop(8, turn)

    send_across(0)
    aggregate(1)

    ra, rb = pl.ds(0, 256), pl.ds(256, 256)
    gat = []
    rel = []
    for cc in (oc, c):
        gat.append(
            [
                [remote(s.at.at[x, cc, part], s.at.at[x, cc, part], xdev(1)) for part in (ra, rb)],
                [remote(s.at.at[x, cc, part], s.at.at[x, cc, part], xdev(-1)) for part in (rb, ra)],
            ]
        )
        rel.append(
            [
                remote(s.at.at[x_l, cc, ra], s.at.at[x_l, cc, ra], xdev(1)),
                remote(s.at.at[x_r, cc, rb], s.at.at[x_r, cc, rb], xdev(-1)),
            ]
        )

    def start_gather(f):
        for k in range(2):
            for d in range(2):
                gat[f][d][k].start()

    def relay(f):
        for d in range(2):
            gat[f][d][0].wait_recv()
            rel[f][d].start()

    start_gather(0)

    for d, yi in enumerate((y_r, y_l)):
        w1c[d].wait_recv()

        def add(q, d=d, yi=yi):
            rows = pl.ds(pl.multiple_of(q * 128, 128), 128)
            s.w[yi, c * 2 + d, rows, :] = (
                s.w[yi, c * 2 + d, rows, :].astype(F32) + s.w1[d, rows, :].astype(F32)
            ).astype(BF)

        loop(4, add)
        wac[d].start()

    for copy in late:
        copy.wait()

    def branch(h):
        for d in range(2):
            nac[h][d].wait_recv()
            agc[h][d].wait_recv()
        z2c[h].wait_recv()
        rows = pl.ds(h * 16, 16)

        def first(q, acc):
            fs = at_step(q)
            up = (
                s.p[zl * 4 + x, h, :, fs].astype(F32)
                + s.xw[0, h, :, fs].astype(F32)
                + s.xw[1, h, :, fs].astype(F32)
                + s.z2[h, :, fs].astype(F32)
            )
            scaled = s.gain[:, fs].astype(F32) * up
            s.scaled[h, :, fs] = scaled
            return acc + lanes(s.hid[rows, fs].astype(F32) * scaled)

        dots = lax.fori_loop(0, NSTEP, first, jnp.zeros((16, 128), F32))
        mean = jnp.sum(dots, axis=1, keepdims=True) / D
        inv = s.inv[rows, 0:1]
        s.coef[h] = jnp.broadcast_to(inv * inv * inv * mean, (16, 128))

    chc = [
        [
            remote(
                s.chs.at[h, :, pl.ds(k * PIECE, PIECE)],
                s.ch.at[h, :, pl.ds(k * PIECE, PIECE)],
                {"section": lax.rem(sec + 3, NS)},
                keep=False,
            )
            for k in range(PIECES)
        ]
        for h in range(2)
    ]

    def chain(h):
        rows = pl.ds(h * 16, 16)
        for k in range(PIECES):

            @pl.when(sec < NS - 1)
            def _():
                chc[h][k].wait_recv()

            inv = s.inv[rows, 0:1]
            coef = s.coef[h, :, 0:1]

            def run(q):
                fs = pl.ds(pl.multiple_of(k * PIECE + q * STEP, STEP), STEP)
                term = inv * s.scaled[h, :, fs] - s.hid[rows, fs].astype(F32) * coef
                term = term + s.ch[h, :, fs].astype(F32)
                s.chs[h, :, fs] = term.astype(BF)
                o_ig[rows, fs] = (term + s.above[rows, fs].astype(F32)).astype(BF)

            loop(PIECE // STEP, run)

            @pl.when(sec > 0)
            def _():
                chc[h][k].start()

    branch(0)

    @pl.when(sec >= 2)
    def _():
        chain(0)

    send_across(1)
    start_gather(1)
    relay(0)

    @pl.when(sec == 1)
    def _():
        chain(0)

    branch(1)

    @pl.when(sec == 3)
    def _():
        chain(1)

    @pl.when(sec == 0)
    def _():
        chain(0)

    relay(1)

    def products(cc, zc, rows):
        total = None
        for xx in range(4):
            left = s.at[xx, cc, rows, :]
            right = s.b[:, zc, xx].reshape(256, 256)
            part = contract(left, right)
            total = part if total is None else total + part
        return total

    for copy in bc:
        copy.wait_recv()

    def arrived(f):
        for d in range(2):
            gat[f][d][1].wait_recv()
            rel[f][d].wait_recv()

    blocks = [pl.ds(0, 256), pl.ds(256, 256)]
    arrived(0)
    gcc = remote(s.gcs, s.gc, cdev)

    def other_core(q):
        rows = pl.ds(pl.multiple_of(lax.rem(q, 2) * 256, 256), 256)
        s.gcs[q // 2, rows, :] = products(oc, q // 2, rows).astype(BF)

    loop(4, other_core)
    gcc.start()

    @pl.when(sec == 2)
    def _():
        chain(1)

    arrived(1)
    gcc.wait_recv()
    gzc = []
    for k, rows in enumerate(blocks):
        s.gzs[k] = (products(c, oz, rows) + s.gc[oz, rows, :].astype(F32)).astype(BF)
        copy = remote(s.gzs.at[k], s.gz.at[k], zdev)
        copy.start()
        gzc.append(copy)
    for rows in blocks:
        s.own[rows, :] = products(c, zl, rows) + s.gc[zl, rows, :].astype(F32)

    @pl.when(sec <= 1)
    def _():
        chain(1)

    for copy in wnc + wac:
        copy.wait_recv()

    def finish(half, rows, base, grad):
        for kv, (oa, om) in enumerate(((o_ak, o_mk), (o_av, o_mv))):
            cols = pl.ds(kv * 128, 128)
            out = pl.ds(pl.multiple_of(half * 512 + base, 128), 128)
            total = (
                s.w[y, c * 2 + half, rows, cols].astype(F32)
                + s.wy[0, half, rows, cols].astype(F32)
                + s.wy[1, half, rows, cols].astype(F32)
            )
            total = total - (inner_rate * FACTOR) * grad[:, kv * 128 : kv * 128 + 128]
            anchor = s.anc[kv, out, :]
            mean = anchor - total * 0.125
            moment = outer_beta * s.mom[kv, out, :] + mean
            om[out, :] = moment
            oa[out, :] = anchor - outer_rate * (mean + outer_beta * moment)

    def finish_own(q):
        rows = pl.ds(pl.multiple_of(q * 128, 128), 128)
        finish(zl, rows, q * 128, s.own[rows, :])

    loop(4, finish_own)
    for copy in gzc:
        copy.wait_recv()

    def finish_other(q):
        rows = pl.ds(pl.multiple_of(q * 128, 128), 128)
        inner = pl.ds(pl.multiple_of(lax.rem(q, 2) * 128, 128), 128)
        finish(oz, rows, q * 128, s.gz[q // 2, inner, :].astype(F32))

    loop(4, finish_other)

    for copy in sent:
        copy.wait_send()

    @pl.when(sec > 0)
    def _():
        for h in range(2):
            for copy in chc[h]:
                copy.wait_send()


def local(hidden, gain, above, kc, vc, wk, wv, ak, av, mk, mv):
    outs = pl.pallas_call(
        kernel,
        out_shape=[jax.ShapeDtypeStruct((1024, 128), F32)] * 4
        + [jax.ShapeDtypeStruct((32, D), BF)],
        in_specs=[pl.BlockSpec(memory_space=pl.ANY)] * 11,
        out_specs=[pl.BlockSpec(memory_space=pltpu.VMEM)] * 5,
        scratch_shapes=[pltpu.VMEM(shape, kind) for shape, kind in SCRATCH.values()]
        + [
            pltpu.SemaphoreType.DMA((NREMOTE,)),
            pltpu.SemaphoreType.DMA((NREMOTE,)),
            pltpu.SemaphoreType.DMA((NLOCAL,)),
        ],
        compiler_params=pltpu.CompilerParams(
            collective_id=0, has_side_effects=True, vmem_limit_bytes=60 * 1024 * 1024
        ),
    )(
        hidden.reshape(32, D),
        gain,
        above.reshape(32, D),
        kc.reshape(TOK, 128),
        vc.reshape(TOK, 128),
        wk.reshape(4, 4, 512, 128),
        wv.reshape(4, 4, 512, 128),
        ak.reshape(1024, 128),
        av.reshape(1024, 128),
        mk.reshape(1024, 128),
        mv.reshape(1024, 128),
    )
    return tuple(o[None] for o in outs[:4]) + (outs[4][None, None],)


def solution(mesh):
    square = P("section", "island", "tensor")
    wide = P("island", "section", None, "tensor")
    return jax.shard_map(
        local,
        mesh=mesh,
        in_specs=(
            P("island", "section", "tensor", None),
            P("section", None),
            P("island", "tensor", None),
            wide,
            wide,
            wide,
            wide,
            square,
            square,
            square,
            square,
        ),
        out_specs=(square, square, square, square, P("island", "section", "tensor", None)),
        check_vma=False,
    )
```
